32 devices in a mesh: dp: 16 (over z, x, core), tp: 2 (over y).
Axes of the slice: x: 2, y: 2, z: 4, core: 2. Of those that a mesh axis runs over, the one named last changes fastest.
Arguments:
- tokens: bfloat16 [4096, 2560], P('dp', 'tp'), may hold values from -16 to 16, as said below
- master: float32 [3, 14336, 2560], P(None, ('dp', 'tp')), may hold values from -1 to 1, as said below
- gradients: bfloat16 [3, 14336, 2560], P(None, ('dp', 'tp')), may hold values from -12 to 12
- first_moment: float32 [3, 14336, 2560], P(None, ('dp', 'tp')), may hold values from -6 to 6
- second_moment: float32 [3, 14336, 2560], P(None, ('dp', 'tp')), may hold values from 1 to 16
- unit_scales: float32 [2, 14336], P(None, ('dp', 'tp')), may hold values from 0.25 to 1.75
- mix_rate: float32 [2560], replicated, may hold values from 0.1 to 0.6
Outputs:
- decoded: bfloat16 [4096, 2560], P('dp', 'tp')
The draws below stay inside these ranges and needn't reach their ends.
Inputs may be any that keep to these rules, and one draw needn't show every extreme that they name: `tokens`: each token's features have root-mean-square close to one. `master`: each row of each of the three matrices has unit length.
All inputs are finite; a program needn't handle non-finite values.
Results may differ from the reference program's by a relative error of at most 0.0085.
Values may be sent and summed in bfloat16 or wider, within the bound.
No kernel may reach another device: no remote copies, remote signals or barrier semaphores. Data moves between devices by JAX's collectives and lax.ppermute only.
A program may use at most 256 MiB of HBM per device.

```python
import math
import jax
import jax.numpy as jnp
from jax import lax

D = 2560
FFW = 14336
TOKENS = 4096


def column_profile(key, spread, width_count):
    ramp_scale = jnp.exp(jnp.log(spread) * (jnp.arange(width_count, dtype=jnp.float32) / (width_count - 1) - 0.5))
    roughness = jax.random.uniform(key, (width_count,), jnp.float32, 0.6, 1.4)
    return ramp_scale * roughness


def draw_tokens(key, part):
    key_base = jax.random.fold_in(key, 11)
    key_profile = jax.random.fold_in(key, 12)
    base_values = jnp.clip(jax.random.normal(key_base, (TOKENS, D), jnp.float32), -5.0, 5.0)
    profile = column_profile(key_profile, 3.0, D)
    values = base_values * profile[None, :]
    values = values / jnp.sqrt(jnp.mean(values * values, axis=1, keepdims=True) + 1e-06)
    return values.astype(jnp.bfloat16)


def draw_master(key, part):
    key_base = jax.random.fold_in(key, 21)
    key_flat = jax.random.fold_in(key, 22)
    key_ramp = jax.random.fold_in(key, 23)
    base_values = jnp.clip(jax.random.normal(key_base, (3, FFW, D), jnp.float32), -5.0, 5.0)
    ramp = column_profile(key_ramp, 3.0, D)
    flat_scale = jax.random.uniform(key_flat, (2, 1, D), jnp.float32, 0.6, 1.4)
    profile = jnp.concatenate([flat_scale, ramp[None, None, :]], axis=0)
    values = base_values * profile
    values = values / jnp.sqrt(jnp.sum(values * values, axis=2, keepdims=True) + 1e-06)
    return values.astype(jnp.float32)


def block_scale(own_key, dims, pieces, smallest, largest):
    level = 1.0
    for dim, parts in pieces:
        heights = jax.random.uniform(jax.random.fold_in(jax.random.fold_in(own_key, 6), dim), (parts,), jnp.float32, smallest / len(pieces), largest / len(pieces))
        level = level * jnp.repeat(jnp.exp(heights), dims[dim] // parts).reshape((-1,) + (1,) * (len(dims) - 1 - dim))
    return level


def noise(stream_key, dims, deviation, most, pieces=(), kind=jnp.bfloat16):
    values = jax.random.normal(stream_key, dims, jnp.float32) * deviation
    if len(pieces) > 0:
        values = block_scale(stream_key, dims, pieces, -0.22, 0.18) * values
    return jnp.clip(values, min=-most, max=most).astype(kind)


def setup_inputs(seed: int = 0) -> dict:
    key_list = jax.random.split(jax.random.key(seed), 8)
    return {
        "tokens": draw_tokens(jax.random.fold_in(key_list[7], 71), 0),
        "master": draw_master(jax.random.fold_in(key_list[7], 71), 0),
        "gradients": noise(key_list[2], (3, FFW, D), 3.0, 12.0, ((1, 32),)),
        "first_moment": noise(key_list[3], (3, FFW, D), 1.0, 6.0, ((1, 32),), jnp.float32),
        "second_moment": jnp.clip(jnp.exp(math.log(16.0) - 2.7725887 * jax.random.uniform(key_list[4], (3, FFW, D), jnp.float32) ** block_scale(key_list[4], (3, FFW, D), ((1, 32),), -0.2, 0.2)), 1.0, 16.0),
        "unit_scales": jnp.clip(1.0 + 0.15 * jax.random.normal(key_list[5], (2, FFW), jnp.float32), 0.25, 1.75),
        "mix_rate": jnp.clip(jax.random.uniform(key_list[6], (D,), jnp.float32, 0.1, 0.6), 0.1, 0.6),
    }


beta_first = 0.9
beta_second = 0.95
learn_rate = 0.02
adam_steps = 20
epsilon = 1e-06

def adam_unit(master, gradients, first_moment, second_moment):
    gradient = gradients.astype(jnp.float32)
    moment_one = beta_first * first_moment + (1.0 - beta_first) * gradient
    moment_two = beta_second * second_moment + (1.0 - beta_second) * gradient * gradient
    stepped = master - learn_rate * (moment_one / (1.0 - beta_first ** adam_steps)) / (jnp.sqrt(moment_two / (1.0 - beta_second ** adam_steps)) + 1e-08)
    lengths = jnp.sqrt(lax.optimization_barrier(jnp.sum(stepped * stepped, axis=-1, keepdims=True)) + epsilon)
    return (stepped / lengths).astype(jnp.bfloat16)

def reference(tokens, master, gradients, first_moment, second_moment, unit_scales, mix_rate):
    unit_rows = adam_unit(master, gradients, first_moment, second_moment)
    scales_bf = lax.optimization_barrier(unit_scales.astype(jnp.bfloat16)).astype(jnp.float32)
    gate_in = jnp.dot(tokens, unit_rows[0].T, preferred_element_type=jnp.float32) * scales_bf[0][None, :]
    up_in = jnp.dot(tokens, unit_rows[1].T, preferred_element_type=jnp.float32) * scales_bf[1][None, :]
    hidden = (jax.nn.silu(gate_in) * up_in).astype(jnp.bfloat16)
    branch = jnp.dot(hidden, unit_rows[2], preferred_element_type=jnp.float32)
    branch_rms = jnp.sqrt(lax.optimization_barrier(jnp.mean(branch * branch, axis=1, keepdims=True)) + epsilon)
    inputs = tokens.astype(jnp.float32)
    mix_rates = mix_rate[None, :]
    mixed_state = inputs + mix_rates * (branch / branch_rms - inputs)
    mixed_rms = jnp.sqrt(lax.optimization_barrier(jnp.mean(mixed_state * mixed_state, axis=1, keepdims=True)) + epsilon)
    return (mixed_state / mixed_rms).astype(jnp.bfloat16)
```

```python
import jax
import jax.numpy as jnp
from jax import lax
from jax.sharding import PartitionSpec as P

beta_first = 0.9
beta_second = 0.95
learn_rate = 0.02
adam_steps = 20
epsilon = 1e-06
chunk_count = 2


def adam_unit(master, gradients, first_moment, second_moment):
    gradient = gradients.astype(jnp.float32)
    moment_one = beta_first * first_moment + (1.0 - beta_first) * gradient
    moment_two = beta_second * second_moment + (1.0 - beta_second) * gradient * gradient
    stepped = master - learn_rate * (moment_one / (1.0 - beta_first**adam_steps)) / (
        jnp.sqrt(moment_two / (1.0 - beta_second**adam_steps)) + 1e-08
    )
    lengths = jnp.sqrt(jnp.sum(stepped * stepped, axis=-1, keepdims=True) + epsilon)
    return stepped / lengths


def largest_divisor(count):
    return max(k for k in range(1, count + 1) if count % k == 0 and k * k <= count)


class Grid:
    def __init__(self, mesh):
        self.dp, self.tp = mesh.shape["dp"], mesh.shape["tp"]
        self.cores = 2 if self.dp % 2 == 0 else 1
        rest = self.dp // self.cores
        self.inner = largest_divisor(rest)
        self.outer = rest // self.inner

    def shift(self, value, outer=0, inner=0, core=0):
        pairs = []
        for z in range(self.outer):
            for x in range(self.inner):
                for c in range(self.cores):
                    to_z, to_x = (z + outer) % self.outer, (x + inner) % self.inner
                    to_c = (c + core) % self.cores
                    pairs.append(
                        (
                            (z * self.inner + x) * self.cores + c,
                            (to_z * self.inner + to_x) * self.cores + to_c,
                        )
                    )
        return lax.ppermute(value, "dp", pairs)

    def z(self, value, steps):
        return self.shift(value, outer=steps) if steps % self.outer else value

    def x(self, value, steps):
        return self.shift(value, inner=steps) if steps % self.inner else value

    def c(self, value, steps):
        return self.shift(value, core=steps) if steps % self.cores else value

    def y(self, value, steps):
        if steps % self.tp == 0:
            return value
        return lax.ppermute(value, "tp", [(t, (t + steps) % self.tp) for t in range(self.tp)])


def gather_chunk(grid, block):
    plane = jnp.concatenate([grid.z(block, s) for s in range(grid.outer)], axis=0)
    half = plane.shape[0] // 2
    pieces = {(0, 0): plane}
    for sx in range(1, grid.inner):
        pieces[sx, 0] = grid.x(plane, sx)
    for sy in range(1, grid.tp):
        pieces[0, sy] = grid.y(plane, sy)
    for sx in range(1, grid.inner):
        for sy in range(1, grid.tp):
            top = grid.x(pieces[0, sy][:half], sx)
            low = grid.y(pieces[sx, 0][half:], sy)
            pieces[sx, sy] = jnp.concatenate([top, low], axis=0)
    return pieces


def hidden_rows(grid, pieces, sx, gate_up):
    total = 0.0
    for sy in range(grid.tp):
        total = total + lax.dot_general(
            pieces[sx, sy],
            gate_up[sy],
            (((1,), (1,)), ((), ())),
            preferred_element_type=jnp.float32,
        )
    units = total.shape[1] // 2
    return (jax.nn.silu(total[:, :units]) * total[:, units:]).astype(jnp.bfloat16)


def scatter_chunk(grid, hidden, down):
    def part(sx, sy):
        return jnp.dot(hidden[sx], down[sy], preferred_element_type=jnp.float32)

    bf16 = jnp.bfloat16
    half = hidden[0].shape[0] // 2
    from_y, from_x = {}, {}
    for sx in range(1, grid.inner):
        for sy in range(1, grid.tp):
            corner = part(sx, sy).astype(bf16)
            from_y.setdefault(sx, []).append(grid.y(corner[:half], -sy))
            from_x.setdefault(sy, []).append(grid.x(corner[half:], -sx))
    received = []
    for sy in range(1, grid.tp):
        sent = part(0, sy)
        low = sent[half:]
        for arrived in from_x.get(sy, []):
            low = low + arrived.astype(jnp.float32)
        sent = jnp.concatenate([sent[:half], low], axis=0).astype(bf16)
        received.append(grid.y(sent, -sy))
    for sx in range(1, grid.inner):
        sent = part(sx, 0)
        top = sent[:half]
        for arrived in from_y.get(sx, []):
            top = top + arrived.astype(jnp.float32)
        sent = jnp.concatenate([top, sent[half:]], axis=0).astype(bf16)
        received.append(grid.x(sent, -sx))
    total = part(0, 0)
    for arrived in received:
        total = total + arrived.astype(jnp.float32)
    rows = total.shape[0] // grid.outer
    shares = total[:rows]
    for s in range(1, grid.outer):
        sent = total[s * rows : (s + 1) * rows].astype(bf16)
        shares = shares + grid.z(sent, -s).astype(jnp.float32)
    return shares


def mix(grid, shares, tokens, mix_rates, model_width):
    inputs_local = tokens.astype(jnp.float32)
    kept_part = (1.0 - mix_rates) * inputs_local
    moved_part = mix_rates * shares
    sums = jnp.stack(
        [
            jnp.sum(shares * shares, axis=1),
            jnp.sum(kept_part * kept_part, axis=1),
            jnp.sum(kept_part * moved_part, axis=1),
            jnp.sum(moved_part * moved_part, axis=1),
        ]
    )
    totals = sums
    for sy in range(1, grid.tp):
        totals = totals + grid.y(sums, sy)
    branch_rms = jnp.sqrt(totals[0] / model_width + epsilon)
    mixed_state = inputs_local + mix_rates * (shares / branch_rms[:, None] - inputs_local)
    mean_square = (
        totals[1] + 2.0 * totals[2] / branch_rms + totals[3] / (branch_rms * branch_rms)
    ) / model_width
    result = mixed_state / jnp.sqrt(mean_square + epsilon)[:, None]
    return result.astype(jnp.bfloat16)


def solution(mesh):
    grid = Grid(mesh)

    def columns(rows, width, sy):
        source = (lax.axis_index("tp") - sy) % grid.tp
        return lax.dynamic_slice_in_dim(rows, source * width, width, rows.ndim - 1)

    def shards(tokens, master, gradients, first_moment, second_moment, unit_scales, mix_rate):
        width = tokens.shape[1]
        model_width = master.shape[2]
        scales_bf = unit_scales.astype(jnp.bfloat16).astype(jnp.float32)
        rows = tokens.shape[0] // chunk_count
        blocks = [tokens[k * rows : (k + 1) * rows] for k in range(chunk_count)]
        gathered = [gather_chunk(grid, block) for block in blocks]

        unit_rows = []
        for k in range(3):
            unit = adam_unit(master[k], gradients[k], first_moment[k], second_moment[k])
            if k < 2:
                unit = unit * scales_bf[k][:, None]
            unit_rows.append(unit.astype(jnp.bfloat16))
        both = [[grid.c(unit, s) for s in range(grid.cores)] for unit in unit_rows]
        gate_up = [
            jnp.concatenate([columns(u, width, sy) for k in range(2) for u in both[k]], axis=0)
            for sy in range(grid.tp)
        ]
        down = [
            jnp.concatenate([columns(u, width, sy) for u in both[2]], axis=0)
            for sy in range(grid.tp)
        ]

        mix_rates = columns(mix_rate, width, 0)[None, :]
        results = []
        for block, pieces in zip(blocks, gathered):
            hidden = [hidden_rows(grid, pieces, sx, gate_up) for sx in range(grid.inner)]
            shares = scatter_chunk(grid, hidden, down)
            results.append(mix(grid, shares, block, mix_rates, model_width))
        return jnp.concatenate(results, axis=0)

    placed = (
        P("dp", "tp"),
        P(None, ("dp", "tp"), None),
        P(None, ("dp", "tp"), None),
        P(None, ("dp", "tp"), None),
        P(None, ("dp", "tp"), None),
        P(None, ("dp", "tp")),
        P(),
    )
    return jax.shard_map(
        shards, mesh=mesh, in_specs=placed, out_specs=P("dp", "tp"), check_vma=False
    )
```
